1024 devices in a mesh: dp: 32 (over y, x_lo), expert: 32 (over z, x_hi, core).
Axes of the slice: x: 8 (x_hi: 2, x_lo: 4; x = x_hi * 4 + x_lo), y: 8, z: 8, core: 2. Of those that a mesh axis runs over, the one named last changes fastest.
Arguments:
- shortcut_in: bfloat16 [512, 7168], P('expert', 'dp'), may hold values from -6 to 6
- current_in: bfloat16 [512, 7168], P('expert', 'dp'), may hold values from -6 to 6
- expert_ids: int32 [512, 8], P('expert'), may hold values from 0 to 31, all different within a row; in each aligned block of 16 rows (0 to 15, 16 to 31, ...) at most 6 rows name the same one
- route_weight: float32 [512, 8], P('expert'), may hold values from 0.1 to 1
- gate_weight: bfloat16 [32, 7168, 2048], P('expert', 'dp'), may hold values from -0.125 to 0.125
- up_weight: bfloat16 [32, 7168, 2048], P('expert', 'dp'), may hold values from -0.125 to 0.125
- down_weight: bfloat16 [32, 2048, 7168], P('expert', None, 'dp'), may hold values from -0.125 to 0.125
- shared_gate: bfloat16 [7168, 2048], P('dp'), may hold values from -0.125 to 0.125
- shared_up: bfloat16 [7168, 2048], P('dp'), may hold values from -0.125 to 0.125
- shared_down: bfloat16 [2048, 7168], P(None, 'dp'), may hold values from -0.125 to 0.125
Outputs:
- mixed: bfloat16 [512, 7168], P('expert', 'dp')
The draws below stay inside these ranges and needn't reach their ends.
Inputs may be any that keep to these rules, and one draw needn't show every extreme that they name: `expert_ids`: each row names 8 different experts. In each aligned block of 16 rows (the tokens of one index of the expert axis) no expert is named by more than 6 rows, and in at least one such block some expert is named by exactly 6 rows.
All inputs are finite; a program needn't handle non-finite values.
Results may differ from the reference program's by a relative error of at most 0.035.
Values may be sent and summed in bfloat16 or wider, within the bound.
No kernel may reach another device: no remote copies, remote signals or barrier semaphores. Data moves between devices by JAX's collectives and lax.ppermute only.
A program may use at most 32 MiB of HBM per device.

```python
import math
import jax
import jax.numpy as jnp
import numpy as np
from jax import lax

D = 7168
H = 2048
TOK_DEV = 16
EXPERTS = 32
TOP = 8
CAP = 6
TOKENS = 512
N_DP = 32
N_EXPERT = 32


def strengthened(array, own_key, source, target, parts, factor):
    owner, partner = [(jnp.arange(array.shape[dim]) // (array.shape[dim] // parts)).reshape([-1 if axis == dim else 1 for axis in range(array.ndim)]) for dim in (source, target)]
    chosen = jax.random.permutation(own_key, parts)[partner]
    strong = (owner == chosen) | (owner == (partner + parts // 2) % parts)
    return jnp.where(strong, factor * array, array)


def shard_levels(key, shape, cuts, least, top_value):
    factor_of, own = 1.0, jax.random.fold_in(key, 6)
    for position, blocks in cuts:
        heights = jnp.exp(jax.random.uniform(jax.random.fold_in(own, position), (blocks,), jnp.float32, least / len(cuts), top_value / len(cuts)))
        factor_of = factor_of * jnp.repeat(heights, shape[position] // blocks).reshape([-1 if axis == position else 1 for axis in range(len(shape))])
    return factor_of


def routed_block(own_key, own, number, rows, amount, top, bound, skew):
    sequence = jax.random.permutation(own_key, amount)
    crowded, common = portions_of(amount, rows * top, bound, skew, True), portions_of(amount, rows * top, bound, skew, False)
    places = jnp.arange(amount)

    def named(tallies, offset_by):
        used = int((tallies > 0).sum())
        fixed = max(1, used // 4)
        shifted = fixed + (places - fixed + offset_by * (used - fixed)) % max(1, amount - fixed)
        return jnp.zeros((amount,), jnp.int32).at[sequence[jnp.where(places < fixed, places, shifted)]].set(jnp.asarray(tallies, jnp.int32))

    tallies = jnp.where(number % 4 == 0, named(crowded, number // 4), named(common, number - number // 4 - 1))
    mixed = jax.random.permutation(jax.random.fold_in(own, 3), amount)
    donor, taker = mixed[0:amount // 2 * 2:2], mixed[1:amount // 2 * 2:2]
    slack = jnp.minimum(tallies[donor] - 1, bound - tallies[taker]) // 2
    slack = jnp.where((donor == sequence[0]) | (taker == sequence[0]) | (tallies[taker] == 0), 0, jnp.maximum(slack, 0))
    shifted = jax.random.randint(jax.random.fold_in(own, 4), (amount // 2,), 0, 1 << 20) % (slack + 1)
    tallies = tallies.at[donor].add(-shifted).at[taker].add(shifted)
    labels = jnp.searchsorted(jnp.cumsum(tallies), jnp.arange(rows * top), side="right").astype(jnp.int32)
    listing = labels.reshape(top, rows).T
    listing = listing[jax.random.permutation(jax.random.fold_in(own, 1), rows)]
    offset_by = jax.random.randint(jax.random.fold_in(own, 2), (rows, 1), 0, top)
    return jnp.take_along_axis(listing, (jnp.arange(top)[None, :] + offset_by) % top, axis=1)


def portions_of(number_of, total, reach, skew, full):
    loads = [(1 << 20) // math.isqrt(grade ** skew) + 1 for grade in range(1, number_of + 1)]
    largest = reach if full else min(reach, max(-(-total // number_of), total * loads[0] // sum(loads)))
    least = 1 if total - largest >= number_of - 1 else 0
    given, surplus = [largest] + [least] * (number_of - 1), total - largest - least * (number_of - 1)
    while surplus > 0:
        movable = [i for i in range(1, number_of) if given[i] < largest] or [i for i in range(1, number_of) if given[i] < reach]
        mass, remaining = sum([loads[i] for i in movable]), surplus
        for i in movable:
            extra = min(reach - given[i], max(1, remaining * loads[i] // mass), surplus)
            given[i] = given[i] + extra
            surplus = surplus - extra
    return np.array(given)


def bell_draw(own_key, shape, spread, most, cuts=(), kind=jnp.bfloat16):
    gain = shard_levels(own_key, shape, cuts, -0.22, 0.18) if cuts else 1.0
    entries = jax.random.normal(own_key, shape, jnp.float32) * spread * gain
    return jnp.minimum(jnp.maximum(entries, -most), most).astype(kind)


def bell_draw_with(rng, shape, width, bound, cuts, heavy, kind=jnp.bfloat16):
    array = width * jax.random.normal(rng, shape, jnp.float32)
    if cuts:
        array = array * shard_levels(rng, shape, cuts, -0.22, 0.18)
    return jnp.clip(strengthened(array, jax.random.fold_in(rng, 3), *heavy), -bound, bound).astype(kind)


def setup_inputs(seed: int = 0) -> dict:
    key_list = jax.random.split(jax.random.key(seed), 11)
    shortcut_in = bell_draw(key_list[0], (TOKENS, D), 1.0, 6.0, ((0, 32), (1, 32)))
    current_in = bell_draw(key_list[1], (TOKENS, D), 1.0, 6.0, ((0, 32), (1, 32)))
    expert_ids_keys = jax.random.split(jax.random.fold_in(key_list[2], 1), TOKENS // TOK_DEV)
    expert_ids_turns = jax.random.permutation(jax.random.fold_in(key_list[2], 3), TOKENS // TOK_DEV)
    expert_ids = jax.vmap(lambda own, number: routed_block(jax.random.fold_in(key_list[2], 2), own, number, TOK_DEV, EXPERTS, TOP, CAP, 2))(expert_ids_keys, expert_ids_turns).reshape((TOKENS, TOP))
    route_weight = jnp.clip(jnp.exp(math.log(1.0) - 2.3025851 * jax.random.uniform(key_list[3], (TOKENS, TOP), jnp.float32) ** shard_levels(key_list[3], (TOKENS, TOP), ((0, 32),), -0.2, 0.2)), 0.1, 1.0)
    gate_weight = bell_draw_with(key_list[4], (EXPERTS, D, H), D ** -0.5, 0.125, ((0, 32), (1, 32)), (1, 2, 32, 2.75))
    up_weight = bell_draw_with(key_list[5], (EXPERTS, D, H), D ** -0.5, 0.125, ((0, 32), (1, 32)), (1, 2, 32, 2.75))
    down_weight = bell_draw(key_list[6], (EXPERTS, H, D), H ** -0.5, 0.125, ((0, 32), (2, 32)))
    shared_gate = bell_draw_with(key_list[7], (D, H), D ** -0.5, 0.125, ((0, 32),), (0, 1, 32, 2.75))
    shared_up = bell_draw_with(key_list[8], (D, H), D ** -0.5, 0.125, ((0, 32),), (0, 1, 32, 2.75))
    shared_down = bell_draw(key_list[9], (H, D), H ** -0.5, 0.125, ((1, 32),))
    return {"shortcut_in": shortcut_in, "current_in": current_in, "expert_ids": expert_ids, "route_weight": route_weight, "gate_weight": gate_weight, "up_weight": up_weight, "down_weight": down_weight, "shared_gate": shared_gate, "shared_up": shared_up, "shared_down": shared_down}


def blocked_product(inputs, weight):
    count = inputs.shape[0]
    block = inputs.shape[1] // N_DP
    pieces = inputs.astype(jnp.float32).reshape(count, N_DP, block)
    blocks = weight.astype(jnp.float32).reshape(N_DP, block, weight.shape[1])
    partial_value = jnp.einsum("rnd,ndh->nrh", pieces, blocks, precision=lax.Precision.HIGHEST)
    rounded = lax.optimization_barrier(partial_value.astype(jnp.bfloat16))
    return jnp.sum(rounded.astype(jnp.float32), axis=0)


def swiglu_hidden(inputs, gate_w, up_w):
    gate = blocked_product(inputs, gate_w)
    upper = blocked_product(inputs, up_w)
    return (jax.nn.silu(gate) * upper).astype(jnp.bfloat16)


def reference(shortcut_in, current_in, expert_ids, route_weight, gate_weight, up_weight, down_weight, shared_gate, shared_up, shared_down):
    count = TOKENS * TOP
    limit = N_EXPERT * CAP
    flat_ids = expert_ids.reshape(-1).astype(jnp.int32)
    flat_tok = jnp.arange(count, dtype=jnp.int32) // TOP
    flat_weight = route_weight.reshape(-1)

    def one_expert(total, inputs):
        gate_w, up_w, down_w, number = inputs
        chosen = flat_ids == number
        rank = jnp.cumsum(chosen.astype(jnp.int32)) - 1
        slots = jnp.where(chosen, rank, limit).astype(jnp.int32)
        source = jnp.zeros((limit,), jnp.int32).at[slots].set(jnp.arange(count, dtype=jnp.int32), mode="drop")
        used = jnp.zeros((limit,), jnp.float32).at[slots].set(1.0, mode="drop")
        token_index = flat_tok[source]
        gathered = shortcut_in[token_index]
        hidden = swiglu_hidden(gathered, gate_w, up_w)
        result = jnp.dot(hidden, down_w, preferred_element_type=jnp.float32).astype(jnp.bfloat16)
        result = lax.optimization_barrier(result).astype(jnp.float32)
        scale = used * flat_weight[source]
        total = total.at[token_index].add(scale[:, None] * result)
        return total, None

    numbers = jnp.arange(EXPERTS, dtype=jnp.int32)
    start = jnp.zeros((TOKENS, D), jnp.float32)
    routed, unused_out = lax.scan(one_expert, start, (gate_weight, up_weight, down_weight, numbers))
    shared_hidden = swiglu_hidden(current_in, shared_gate, shared_up)
    shared_out = jnp.dot(shared_hidden, shared_down, preferred_element_type=jnp.float32)
    return (shared_out + routed).astype(jnp.bfloat16)
```

```python
import jax
import jax.numpy as jnp
from jax import lax
from jax.experimental import pallas as pl
from jax.experimental.pallas import tpu as pltpu
from jax.sharding import PartitionSpec as P

F32 = jnp.float32
BF16 = jnp.bfloat16
LANES = 128
SUB = 8
WIDE = 256


def iota(shape, dim):
    return lax.broadcasted_iota(jnp.int32, shape, dim)


def dot(a, b, dims=((1,), (0,)), precision=None):
    return lax.dot_general(a, b, (dims, ((), ())), precision=precision, preferred_element_type=F32)


def pick_rows(rows, padded, cap):
    r = iota((rows, padded), 0)
    p = iota((rows, padded), 1)
    low = p & (SUB - 1)
    hit = (r == cap * (p >> 3) + low) & (low < cap)
    return jnp.where(hit, 1.0, 0.0).astype(BF16)


def pack_body(cap, ids, weight, routed_in, shared_in, out, mix, wide_r, wide_s):
    top, tokens = ids.shape
    experts = out.shape[0] // SUB
    width = routed_in.shape[1]
    ident = ids[...]
    scale = weight[...]
    e_of = iota((experts, tokens), 0)
    named = jnp.zeros((experts, tokens), F32)
    gains = jnp.zeros((experts, tokens), F32)
    for k in range(top):
        same = e_of == ident[k : k + 1, :]
        named = named + jnp.where(same, 1.0, 0.0)
        gains = gains + jnp.where(same, scale[k : k + 1, :], 0.0)
    row = iota((tokens, tokens), 0)
    col = iota((tokens, tokens), 1)
    rank = dot(named, jnp.where(row < col, 1.0, 0.0))
    count = dot(named, jnp.ones((tokens, tokens), F32))
    free = cap - count
    row = iota((experts, experts), 0)
    col = iota((experts, experts), 1)
    before = dot(jnp.where(col < row, 1.0, 0.0), free)
    tok = iota((experts, tokens), 1).astype(F32) - before
    fits = (tok >= 0.0) & (tok < free)
    slot_r = jnp.where(named > 0.0, rank, -1.0)
    slot_s = jnp.where(fits, count + tok, -1.0)

    def spread(a):
        a = jnp.broadcast_to(a[:, None, :], (experts, SUB, tokens))
        return a.reshape(experts * SUB, tokens)

    place = (iota((experts * SUB, tokens), 0) & (SUB - 1)).astype(F32)
    put_r = spread(slot_r) == place
    put_s = jnp.where(spread(slot_s) == place, 1.0, 0.0)
    mix[...] = jnp.where(put_r, spread(gains), put_s)
    wide_r[...] = jnp.zeros_like(wide_r)
    wide_s[...] = jnp.ones_like(wide_s)
    wide_r[:, :width] = routed_in[...]
    wide_s[:, :width] = shared_in[...]
    sent = dot(jnp.where(put_r, 1.0, 0.0).astype(BF16), wide_r[...])
    sent = sent + dot(put_s.astype(BF16), wide_s[...])
    out[...] = sent.astype(BF16)


def up_body(cap, arrived, gate_w, up_w, shared_gate, shared_up, out, left, right):
    padded, wide = arrived.shape
    width, units = gate_w.shape
    rows = padded // SUB * cap
    half = rows // 2
    compact = dot(pick_rows(rows, padded, cap), arrived[...])
    shared = compact[:, width : width + 1] > 0.5
    left[...] = jnp.where(shared, 0.0, compact).astype(BF16)[:, :width]
    right[...] = jnp.where(shared, compact, 0.0).astype(BF16)[:, :width]
    step = 2 * LANES
    for c in range(units // step):
        cols = slice(c * step, (c + 1) * step)
        for which, (w, s) in enumerate(((gate_w, shared_gate), (up_w, shared_up))):
            value = dot(left[...], w[:, cols]) + dot(right[...], s[:, cols])
            value = value.astype(BF16)
            for b in range(2):
                for j in range(2):
                    owner = 2 * (2 * c + b) + j
                    out[owner, which * half : (which + 1) * half, :] = value[
                        j * half : (j + 1) * half, b * LANES : (b + 1) * LANES
                    ]


def act_body(parts, out):
    sources, both, _ = parts.shape
    half = both // 2
    gate = jnp.zeros((half, LANES), F32)
    upper = jnp.zeros((half, LANES), F32)
    for s in range(sources):
        gate = gate + parts[s, :half, :].astype(F32)
        upper = upper + parts[s, half:, :].astype(F32)
    hidden = (jax.nn.silu(gate) * upper).astype(BF16)
    for s in range(sources):
        out[s] = hidden


def down_body(cap, hidden, arrived, down_t, shared_down_t, out, joined):
    owners, half, _ = hidden.shape
    padded = arrived.shape[0]
    width = down_t.shape[0]
    rows = 2 * half
    for owner in range(owners):
        i, j = owner // 2, owner % 2
        joined[j * half : (j + 1) * half, i * LANES : (i + 1) * LANES] = hidden[owner]
    last = ((1,), (1,))
    own = dot(joined[...], down_t[...], last).astype(BF16)
    common = dot(joined[...], shared_down_t[...], last).astype(BF16)
    back = pick_rows(rows, padded, cap)
    first = ((0,), (0,))
    own = dot(back, own, first)
    common = dot(back, common, first)
    shared = arrived[:, width:].astype(F32)[:, :1] > 0.5
    out[...] = jnp.where(shared, common, own).astype(BF16)


def mix_body(returned, mix, out):
    value = dot(mix[...], returned[...].astype(F32), ((0,), (0,)), lax.Precision.HIGHEST)
    out[...] = value.astype(BF16)


def call(body, shape, dtype, *args, scratch=()):
    single = isinstance(dtype, tuple)
    outs = [jax.ShapeDtypeStruct(s, d) for s, d in zip(shape, dtype)] if single else jax.ShapeDtypeStruct(shape, dtype)
    return pl.pallas_call(body, out_shape=outs, scratch_shapes=list(scratch))(*args)


def local(
    shortcut_in,
    current_in,
    expert_ids,
    route_weight,
    gate_weight,
    up_weight,
    down_weight,
    shared_gate,
    shared_up,
    shared_down,
):
    sources = lax.axis_size("expert")
    owners = lax.axis_size("dp")
    tokens, top = expert_ids.shape
    cap = 3 * tokens * top // (2 * sources)
    width = shortcut_in.shape[1]
    units = gate_weight.shape[2]
    padded = sources * SUB
    rows = sources * cap
    sent, mix = call(
        lambda *r: pack_body(cap, *r),
        ((padded, WIDE), (padded, tokens)),
        (BF16, F32),
        expert_ids.T,
        route_weight.T,
        shortcut_in,
        current_in,
        scratch=(pltpu.VMEM((tokens, WIDE), BF16), pltpu.VMEM((tokens, WIDE), BF16)),
    )
    arrived = lax.all_to_all(sent.reshape(sources, SUB, WIDE), "expert", 0, 0, tiled=True)
    arrived = arrived.reshape(padded, WIDE)
    parts = call(
        lambda *r: up_body(cap, *r),
        (owners, rows, LANES),
        BF16,
        arrived,
        gate_weight[0],
        up_weight[0],
        shared_gate,
        shared_up,
        scratch=(pltpu.VMEM((rows, width), BF16), pltpu.VMEM((rows, width), BF16)),
    )
    parts = lax.all_to_all(parts, "dp", 0, 0, tiled=True)
    copies = call(act_body, (owners, rows // 2, LANES), BF16, parts)
    hidden = lax.all_to_all(copies, "dp", 0, 0, tiled=True)
    results = call(
        lambda *r: down_body(cap, *r),
        (padded, width),
        BF16,
        hidden,
        arrived,
        down_weight[0].T,
        shared_down.T,
        scratch=(pltpu.VMEM((rows, units), BF16),),
    )
    returned = lax.all_to_all(results.reshape(sources, SUB, width), "expert", 0, 0, tiled=True)
    return call(mix_body, (tokens, width), BF16, returned.reshape(padded, width), mix)


def solution(mesh):
    placed = (
        P("expert", "dp"),
        P("expert", "dp"),
        P("expert", None),
        P("expert", None),
        P("expert", "dp", None),
        P("expert", "dp", None),
        P("expert", None, "dp"),
        P("dp", None),
        P("dp", None),
        P(None, "dp"),
    )
    return jax.shard_map(
        local, mesh=mesh, in_specs=placed, out_specs=P("expert", "dp"), check_vma=False
    )
```

```python
import jax
import jax.numpy as jnp
from jax import lax
from jax.experimental import pallas as pl
from jax.experimental.pallas import tpu as pltpu
from jax.sharding import PartitionSpec as P

F32 = jnp.float32
BF16 = jnp.bfloat16
LANES = 128
SUB = 8
EARLY = 1 << 34
NEAR = 4
GRANT = 16 << 20
WIDE = 256


def iota(shape, dim):
    return lax.broadcasted_iota(jnp.int32, shape, dim)


def dot(a, b, dims=((1,), (0,)), precision=None):
    return lax.dot_general(a, b, (dims, ((), ())), precision=precision, preferred_element_type=F32)


def pick_rows(rows, padded, cap):
    r = iota((rows, padded), 0)
    p = iota((rows, padded), 1)
    low = p & (SUB - 1)
    hit = (r == cap * (p >> 3) + low) & (low < cap)
    return jnp.where(hit, 1.0, 0.0).astype(BF16)


def pack_body(cap, ids_h, weight_h, routed_h, shared_h, out, mix, ids, weight, routed_in, shared_in, wide_r, wide_s, sems):
    pairs = ((ids_h, ids), (weight_h, weight), (routed_h, routed_in), (shared_h, shared_in))
    copies = [pltpu.make_async_copy(a, b, sems.at[n]) for n, (a, b) in enumerate(pairs)]
    for c in copies:
        c.start()
    for c in copies:
        c.wait()
    top, tokens = ids.shape
    experts = out.shape[0] // SUB
    width = routed_in.shape[1]
    ident = ids[...]
    scale = weight[...]
    e_of = iota((experts, tokens), 0)
    named = jnp.zeros((experts, tokens), F32)
    gains = jnp.zeros((experts, tokens), F32)
    for k in range(top):
        same = e_of == ident[k : k + 1, :]
        named = named + jnp.where(same, 1.0, 0.0)
        gains = gains + jnp.where(same, scale[k : k + 1, :], 0.0)
    row = iota((tokens, tokens), 0)
    col = iota((tokens, tokens), 1)
    rank = dot(named, jnp.where(row < col, 1.0, 0.0))
    count = dot(named, jnp.ones((tokens, tokens), F32))
    free = cap - count
    row = iota((experts, experts), 0)
    col = iota((experts, experts), 1)
    before = dot(jnp.where(col < row, 1.0, 0.0), free)
    tok = iota((experts, tokens), 1).astype(F32) - before
    fits = (tok >= 0.0) & (tok < free)
    slot_r = jnp.where(named > 0.0, rank, -1.0)
    slot_s = jnp.where(fits, count + tok, -1.0)

    def spread(a):
        a = jnp.broadcast_to(a[:, None, :], (experts, SUB, tokens))
        return a.reshape(experts * SUB, tokens)

    place = (iota((experts * SUB, tokens), 0) & (SUB - 1)).astype(F32)
    put_r = spread(slot_r) == place
    put_s = jnp.where(spread(slot_s) == place, 1.0, 0.0)
    mix[...] = jnp.where(put_r, spread(gains), put_s)
    wide_r[...] = jnp.zeros_like(wide_r)
    wide_s[...] = jnp.ones_like(wide_s)
    wide_r[:, :width] = routed_in[...]
    wide_s[:, :width] = shared_in[...]
    sent = dot(jnp.where(put_r, 1.0, 0.0).astype(BF16), wide_r[...])
    sent = sent + dot(put_s.astype(BF16), wide_s[...])
    out[...] = sent.astype(BF16)


def up_body(cap, arrived, gate_w, up_w, shared_gate, shared_up, out, left, right):
    padded, wide = arrived.shape
    width, units = gate_w.shape
    rows = padded // SUB * cap
    half = rows // 2
    compact = dot(pick_rows(rows, padded, cap), arrived[...])
    shared = compact[:, width : width + 1] > 0.5
    left[...] = jnp.where(shared, 0.0, compact).astype(BF16)[:, :width]
    right[...] = jnp.where(shared, compact, 0.0).astype(BF16)[:, :width]
    odd = lax.axis_index("expert") % 2 == 1
    step = 2 * LANES
    for c in range(units // step):
        cols = slice(c * step, (c + 1) * step)
        for which, (w, s) in enumerate(((gate_w, shared_gate), (up_w, shared_up))):
            value = dot(left[...], w[:, cols]) + dot(right[...], s[:, cols])
            value = value.astype(BF16)
            for b in range(2):
                for j in range(2):
                    owner = 2 * (2 * c + b) + j
                    swapped = owner % NEAR * (out.shape[0] // NEAR) + owner // NEAR
                    out[jnp.where(odd, swapped, owner), which * half : (which + 1) * half, :] = value[
                        j * half : (j + 1) * half, b * LANES : (b + 1) * LANES
                    ]


def add_body(parts, out):
    for q in range(out.shape[0]):
        total = parts[0, q].astype(F32)
        for s in range(1, parts.shape[0]):
            total = total + parts[s, q].astype(F32)
        out[q] = total.astype(BF16)


def act_body(parts, out):
    sources, both, _ = parts.shape
    half = both // 2
    gate = jnp.zeros((half, LANES), F32)
    upper = jnp.zeros((half, LANES), F32)
    for s in range(sources):
        gate = gate + parts[s, :half, :].astype(F32)
        upper = upper + parts[s, half:, :].astype(F32)
    hidden = (jax.nn.silu(gate) * upper).astype(BF16)
    for s in range(out.shape[0]):
        out[s] = hidden


def down_body(cap, hidden, arrived, down_t, shared_down_t, out, joined):
    owners, half, _ = hidden.shape
    padded = arrived.shape[0]
    width = down_t.shape[0]
    rows = 2 * half
    for owner in range(owners):
        i, j = owner // 2, owner % 2
        joined[j * half : (j + 1) * half, i * LANES : (i + 1) * LANES] = hidden[owner]
    last = ((1,), (1,))
    own = dot(joined[...], down_t[...], last).astype(BF16)
    common = dot(joined[...], shared_down_t[...], last).astype(BF16)
    back = pick_rows(rows, padded, cap)
    first = ((0,), (0,))
    own = dot(back, own, first)
    common = dot(back, common, first)
    shared = arrived[:, width:].astype(F32)[:, :1] > 0.5
    out[...] = jnp.where(shared, common, own).astype(BF16)


def mix_body(returned, mix, out):
    value = dot(mix[...], returned[...].astype(F32), ((0,), (0,)), lax.Precision.HIGHEST)
    out[...] = value.astype(BF16)


def call(body, shape, dtype, *args, scratch=(), in_hbm=0, flops=0):
    several = isinstance(dtype, tuple)
    outs = [jax.ShapeDtypeStruct(a, d) for a, d in zip(shape, dtype)] if several else jax.ShapeDtypeStruct(shape, dtype)
    hbm, vmem = pl.BlockSpec(memory_space=pltpu.HBM), pl.BlockSpec(memory_space=pltpu.VMEM)
    return pl.pallas_call(
        body,
        out_shape=outs,
        in_specs=[hbm if n < in_hbm else vmem for n in range(len(args))],
        scratch_shapes=list(scratch),
        compiler_params=pltpu.CompilerParams(vmem_limit_bytes=GRANT),
        cost_estimate=pl.CostEstimate(flops=flops, bytes_accessed=0, transcendentals=0) if flops else None,
    )(*[pltpu.with_memory_space_constraint(a, pltpu.HBM) if n < in_hbm else a for n, a in enumerate(args)])


def stage_groups(owners, experts):
    down, across = owners // NEAR, NEAR
    rank = lambda y, x, e: (y * across + x) * experts + e
    first, second = [], []
    for e in range(experts):
        if e % 2:
            first += [[rank(y, x, e) for x in range(across)] for y in range(down)]
            second += [[rank(y, x, e) for y in range(down)] for x in range(across)]
        else:
            first += [[rank(2 * i + h, x, e) for i in range(down // 2)] for h in range(2) for x in range(across)]
            second += [[rank(2 * i + h, x, e) for h in range(2) for x in range(across)] for i in range(down // 2)]
    return first, second


def exchange(array, groups):
    return lax.all_to_all(array, ("dp", "expert"), 0, 0, tiled=True, axis_index_groups=groups)


def local(
    shortcut_in,
    current_in,
    expert_ids,
    route_weight,
    gate_weight,
    up_weight,
    down_weight,
    shared_gate,
    shared_up,
    shared_down,
):
    sources = lax.axis_size("expert")
    owners = lax.axis_size("dp")
    tokens, top = expert_ids.shape
    cap = 3 * tokens * top // (2 * sources)
    width = shortcut_in.shape[1]
    units = gate_weight.shape[2]
    padded = sources * SUB
    rows = sources * cap
    sent, mix = call(
        lambda *r: pack_body(cap, *r),
        ((padded, WIDE), (padded, tokens)),
        (BF16, F32),
        expert_ids.T,
        route_weight.T,
        shortcut_in,
        current_in,
        in_hbm=4,
        flops=EARLY,
        scratch=(
            pltpu.VMEM((top, tokens), jnp.int32),
            pltpu.VMEM((top, tokens), F32),
            pltpu.VMEM((tokens, width), BF16),
            pltpu.VMEM((tokens, width), BF16),
            pltpu.VMEM((tokens, WIDE), BF16),
            pltpu.VMEM((tokens, WIDE), BF16),
            pltpu.SemaphoreType.DMA((4,)),
        ),
    )
    arrived = lax.all_to_all(sent.reshape(sources, SUB, WIDE), "expert", 0, 0, tiled=True)
    arrived = arrived.reshape(padded, WIDE)
    parts = call(
        lambda *r: up_body(cap, *r),
        (owners, rows, LANES),
        BF16,
        arrived,
        gate_weight[0],
        up_weight[0],
        shared_gate,
        shared_up,
        scratch=(pltpu.VMEM((rows, width), BF16), pltpu.VMEM((rows, width), BF16)),
    )
    first, second = stage_groups(owners, sources)
    far = owners // NEAR
    parts = exchange(parts.reshape(NEAR, far * rows, LANES), first)
    parts = call(add_body, (far, rows, LANES), BF16, parts.reshape(NEAR, far, rows, LANES))
    parts = exchange(parts, second)
    copies = call(act_body, (owners, rows // 2, LANES), BF16, parts)
    hidden = lax.all_to_all(copies, "dp", 0, 0, tiled=True)
    results = call(
        lambda *r: down_body(cap, *r),
        (padded, width),
        BF16,
        hidden,
        arrived,
        down_weight[0].T,
        shared_down.T,
        scratch=(pltpu.VMEM((rows, units), BF16),),
    )
    returned = lax.all_to_all(results.reshape(sources, SUB, width), "expert", 0, 0, tiled=True)
    return call(mix_body, (tokens, width), BF16, returned.reshape(padded, width), mix)


def solution(mesh):
    placed = (
        P("expert", "dp"),
        P("expert", "dp"),
        P("expert", None),
        P("expert", None),
        P("expert", "dp", None),
        P("expert", "dp", None),
        P("expert", None, "dp"),
        P("dp", None),
        P("dp", None),
        P(None, "dp"),
    )
    return jax.shard_map(
        local, mesh=mesh, in_specs=placed, out_specs=P("expert", "dp"), check_vma=False
    )
```

```python
import jax
import jax.numpy as jnp
from jax import lax
from jax.experimental import pallas as pl
from jax.experimental.pallas import tpu as pltpu
from jax.sharding import PartitionSpec as P

F32 = jnp.float32
BF16 = jnp.bfloat16
LANES = 128
SUB = 8
EARLY = 1 << 34
RING = ((0, 1, 3, 6), (7, 2, 4, 5))
NEAR = 4
GRANT = 16 << 20
WIDE = 256


def iota(shape, dim):
    return lax.broadcasted_iota(jnp.int32, shape, dim)


def dot(a, b, dims=((1,), (0,)), precision=None):
    return lax.dot_general(a, b, (dims, ((), ())), precision=precision, preferred_element_type=F32)


def pick_rows(rows, padded, cap):
    r = iota((rows, padded), 0)
    p = iota((rows, padded), 1)
    low = p & (SUB - 1)
    hit = (r == cap * (p >> 3) + low) & (low < cap)
    return jnp.where(hit, 1.0, 0.0).astype(BF16)


def pack_body(cap, ids_h, weight_h, routed_h, shared_h, out, mix, ids, weight, routed_in, shared_in, wide_r, wide_s, sems):
    pairs = ((ids_h, ids), (weight_h, weight), (routed_h, routed_in), (shared_h, shared_in))
    copies = [pltpu.make_async_copy(a, b, sems.at[n]) for n, (a, b) in enumerate(pairs)]
    for c in copies:
        c.start()
    for c in copies:
        c.wait()
    top, tokens = ids.shape
    experts = out.shape[0] // SUB
    width = routed_in.shape[1]
    ident = ids[...]
    scale = weight[...]
    e_of = iota((experts, tokens), 0)
    named = jnp.zeros((experts, tokens), F32)
    gains = jnp.zeros((experts, tokens), F32)
    for k in range(top):
        same = e_of == ident[k : k + 1, :]
        named = named + jnp.where(same, 1.0, 0.0)
        gains = gains + jnp.where(same, scale[k : k + 1, :], 0.0)
    row = iota((tokens, tokens), 0)
    col = iota((tokens, tokens), 1)
    rank = dot(named, jnp.where(row < col, 1.0, 0.0))
    count = dot(named, jnp.ones((tokens, tokens), F32))
    free = cap - count
    row = iota((experts, experts), 0)
    col = iota((experts, experts), 1)
    before = dot(jnp.where(col < row, 1.0, 0.0), free)
    tok = iota((experts, tokens), 1).astype(F32) - before
    fits = (tok >= 0.0) & (tok < free)
    slot_r = jnp.where(named > 0.0, rank, -1.0)
    slot_s = jnp.where(fits, count + tok, -1.0)

    def spread(a):
        a = jnp.broadcast_to(a[:, None, :], (experts, SUB, tokens))
        return a.reshape(experts * SUB, tokens)

    place = (iota((experts * SUB, tokens), 0) & (SUB - 1)).astype(F32)
    put_r = spread(slot_r) == place
    put_s = jnp.where(spread(slot_s) == place, 1.0, 0.0)
    mix[...] = jnp.where(put_r, spread(gains), put_s)
    wide_r[...] = jnp.zeros_like(wide_r)
    wide_s[...] = jnp.ones_like(wide_s)
    wide_r[:, :width] = routed_in[...]
    wide_s[:, :width] = shared_in[...]
    sent = dot(jnp.where(put_r, 1.0, 0.0).astype(BF16), wide_r[...])
    sent = sent + dot(put_s.astype(BF16), wide_s[...])
    out[...] = sent.astype(BF16)


def up_body(cap, chunks, arrived, gate_w, up_w, shared_gate, shared_up, out, left, right):
    padded, wide = arrived.shape
    width, units = gate_w.shape
    rows = padded // SUB * cap
    half = rows // 2
    compact = dot(pick_rows(rows, padded, cap), arrived[...])
    shared = compact[:, width : width + 1] > 0.5
    left[...] = jnp.where(shared, 0.0, compact).astype(BF16)[:, :width]
    right[...] = jnp.where(shared, compact, 0.0).astype(BF16)[:, :width]
    odd = lax.axis_index("expert") % 2 == 1
    step = 2 * LANES
    for c in range(units // step):
        cols = slice(c * step, (c + 1) * step)
        for which, (w, s) in enumerate(((gate_w, shared_gate), (up_w, shared_up))):
            value = dot(left[...], w[:, cols]) + dot(right[...], s[:, cols])
            value = value.astype(BF16)
            for b in range(2):
                for j in range(2):
                    owner = 2 * (2 * c + b) + j
                    out[jnp.where(odd, chunks[1][owner], chunks[0][owner]), which * half : (which + 1) * half, :] = value[
                        j * half : (j + 1) * half, b * LANES : (b + 1) * LANES
                    ]


def add_body(parts, out):
    for q in range(out.shape[0]):
        total = parts[0, q].astype(F32)
        for s in range(1, parts.shape[0]):
            total = total + parts[s, q].astype(F32)
        out[q] = total.astype(BF16)


def act_body(parts, out):
    sources, both, _ = parts.shape
    half = both // 2
    gate = jnp.zeros((half, LANES), F32)
    upper = jnp.zeros((half, LANES), F32)
    for s in range(sources):
        gate = gate + parts[s, :half, :].astype(F32)
        upper = upper + parts[s, half:, :].astype(F32)
    hidden = (jax.nn.silu(gate) * upper).astype(BF16)
    for s in range(out.shape[0]):
        out[s] = hidden


def down_body(cap, hidden, arrived, down_t, shared_down_t, out, joined):
    owners, half, _ = hidden.shape
    padded = arrived.shape[0]
    width = down_t.shape[0]
    rows = 2 * half
    for owner in range(owners):
        i, j = owner // 2, owner % 2
        joined[j * half : (j + 1) * half, i * LANES : (i + 1) * LANES] = hidden[owner]
    last = ((1,), (1,))
    own = dot(joined[...], down_t[...], last).astype(BF16)
    common = dot(joined[...], shared_down_t[...], last).astype(BF16)
    back = pick_rows(rows, padded, cap)
    first = ((0,), (0,))
    own = dot(back, own, first)
    common = dot(back, common, first)
    shared = arrived[:, width:].astype(F32)[:, :1] > 0.5
    out[...] = jnp.where(shared, common, own).astype(BF16)


def mix_body(returned, mix, out):
    value = dot(mix[...], returned[...].astype(F32), ((0,), (0,)), lax.Precision.HIGHEST)
    out[...] = value.astype(BF16)


def call(body, shape, dtype, *args, scratch=(), in_hbm=0, flops=0):
    several = isinstance(dtype, tuple)
    outs = [jax.ShapeDtypeStruct(a, d) for a, d in zip(shape, dtype)] if several else jax.ShapeDtypeStruct(shape, dtype)
    hbm, vmem = pl.BlockSpec(memory_space=pltpu.HBM), pl.BlockSpec(memory_space=pltpu.VMEM)
    return pl.pallas_call(
        body,
        out_shape=outs,
        in_specs=[hbm if n < in_hbm else vmem for n in range(len(args))],
        scratch_shapes=list(scratch),
        compiler_params=pltpu.CompilerParams(vmem_limit_bytes=GRANT),
        cost_estimate=pl.CostEstimate(flops=flops, bytes_accessed=0, transcendentals=0) if flops else None,
    )(*[pltpu.with_memory_space_constraint(a, pltpu.HBM) if n < in_hbm else a for n, a in enumerate(args)])


def stage_groups(owners, experts):
    down, across = owners // NEAR, NEAR
    assert down == 2 * NEAR and across == NEAR
    stages = ([], [])
    chunks = [[0] * owners, [0] * owners]
    for e in range(experts):
        if e % 2 == 0:
            one = [[(y, x) for x in range(across)] for y in range(down)]
            two = [[(y, x) for y in range(down)] for x in range(across)]
        else:
            one = [[(y, x) for y in line] for line in RING for x in range(across)]
            two = [[(y, x) for y in pair for x in range(across)] for pair in zip(*RING)]
        place = [{d: group.index(d) for group in stage for d in group} for stage in (one, two)]
        for y in range(down):
            for x in range(across):
                a, b = (p[y, x] for p in place)
                chunks[e % 2][y * across + x] = a * down + b
        for groups, stage in zip(stages, (one, two)):
            groups += [[(y * across + x) * experts + e for y, x in group] for group in stage]
    return stages, chunks


def exchange(array, groups):
    return lax.all_to_all(array, ("dp", "expert"), 0, 0, tiled=True, axis_index_groups=groups)


def local(
    shortcut_in,
    current_in,
    expert_ids,
    route_weight,
    gate_weight,
    up_weight,
    down_weight,
    shared_gate,
    shared_up,
    shared_down,
):
    sources = lax.axis_size("expert")
    owners = lax.axis_size("dp")
    tokens, top = expert_ids.shape
    cap = 3 * tokens * top // (2 * sources)
    width = shortcut_in.shape[1]
    units = gate_weight.shape[2]
    padded = sources * SUB
    rows = sources * cap
    sent, mix = call(
        lambda *r: pack_body(cap, *r),
        ((padded, WIDE), (padded, tokens)),
        (BF16, F32),
        expert_ids.T,
        route_weight.T,
        shortcut_in,
        current_in,
        in_hbm=4,
        flops=EARLY,
        scratch=(
            pltpu.VMEM((top, tokens), jnp.int32),
            pltpu.VMEM((top, tokens), F32),
            pltpu.VMEM((tokens, width), BF16),
            pltpu.VMEM((tokens, width), BF16),
            pltpu.VMEM((tokens, WIDE), BF16),
            pltpu.VMEM((tokens, WIDE), BF16),
            pltpu.SemaphoreType.DMA((4,)),
        ),
    )
    arrived = lax.all_to_all(sent.reshape(sources, SUB, WIDE), "expert", 0, 0, tiled=True)
    arrived = arrived.reshape(padded, WIDE)
    (one, two), chunks = stage_groups(owners, sources)
    parts = call(
        lambda *r: up_body(cap, chunks, *r),
        (owners, rows, LANES),
        BF16,
        arrived,
        gate_weight[0],
        up_weight[0],
        shared_gate,
        shared_up,
        scratch=(pltpu.VMEM((rows, width), BF16), pltpu.VMEM((rows, width), BF16)),
    )
    left = owners // NEAR
    parts = exchange(parts.reshape(NEAR, left * rows, LANES), one)
    parts = call(add_body, (left, rows, LANES), BF16, parts.reshape(NEAR, left, rows, LANES))
    parts = exchange(parts, two)
    copies = call(act_body, (owners, rows // 2, LANES), BF16, parts)
    hidden = lax.all_to_all(copies, "dp", 0, 0, tiled=True)
    results = call(
        lambda *r: down_body(cap, *r),
        (padded, width),
        BF16,
        hidden,
        arrived,
        down_weight[0].T,
        shared_down.T,
        scratch=(pltpu.VMEM((rows, units), BF16),),
    )
    returned = lax.all_to_all(results.reshape(sources, SUB, width), "expert", 0, 0, tiled=True)
    return call(mix_body, (tokens, width), BF16, returned.reshape(padded, width), mix)


def solution(mesh):
    placed = (
        P("expert", "dp"),
        P("expert", "dp"),
        P("expert", None),
        P("expert", None),
        P("expert", "dp", None),
        P("expert", "dp", None),
        P("expert", None, "dp"),
        P("dp", None),
        P("dp", None),
        P(None, "dp"),
    )
    return jax.shard_map(
        local, mesh=mesh, in_specs=placed, out_specs=P("expert", "dp"), check_vma=False
    )
```

```python
import jax
import jax.numpy as jnp
from jax import lax
from jax.experimental import pallas as pl
from jax.experimental.pallas import tpu as pltpu
from jax.sharding import PartitionSpec as P

F32 = jnp.float32
BF16 = jnp.bfloat16
LANES = 128
SUB = 8
EARLY = 1 << 34
RING = ((0, 1, 3, 6), (7, 2, 4, 5))
NEAR = 4
GRANT = 16 << 20
WIDE = 256


def iota(shape, dim):
    return lax.broadcasted_iota(jnp.int32, shape, dim)


def dot(a, b, dims=((1,), (0,)), precision=None):
    return lax.dot_general(a, b, (dims, ((), ())), precision=precision, preferred_element_type=F32)


def pick_rows(rows, padded, cap):
    r = iota((rows, padded), 0)
    p = iota((rows, padded), 1)
    low = p & (SUB - 1)
    hit = (r == cap * (p >> 3) + low) & (low < cap)
    return jnp.where(hit, 1.0, 0.0).astype(BF16)


def pack_body(cap, ids_h, weight_h, routed_h, shared_h, out, mix, ids, weight, routed_in, shared_in, wide_r, wide_s, sems):
    pairs = ((ids_h, ids), (weight_h, weight), (routed_h, routed_in), (shared_h, shared_in))
    copies = [pltpu.make_async_copy(a, b, sems.at[n]) for n, (a, b) in enumerate(pairs)]
    for c in copies:
        c.start()
    for c in copies:
        c.wait()
    top, tokens = ids.shape
    experts = out.shape[0] // SUB
    width = routed_in.shape[1]
    ident = ids[...]
    scale = weight[...]
    e_of = iota((experts, tokens), 0)
    named = jnp.zeros((experts, tokens), F32)
    gains = jnp.zeros((experts, tokens), F32)
    for k in range(top):
        same = e_of == ident[k : k + 1, :]
        named = named + jnp.where(same, 1.0, 0.0)
        gains = gains + jnp.where(same, scale[k : k + 1, :], 0.0)
    row = iota((tokens, tokens), 0)
    col = iota((tokens, tokens), 1)
    rank = dot(named, jnp.where(row < col, 1.0, 0.0))
    count = dot(named, jnp.ones((tokens, tokens), F32))
    free = cap - count
    row = iota((experts, experts), 0)
    col = iota((experts, experts), 1)
    before = dot(jnp.where(col < row, 1.0, 0.0), free)
    tok = iota((experts, tokens), 1).astype(F32) - before
    fits = (tok >= 0.0) & (tok < free)
    slot_r = jnp.where(named > 0.0, rank, -1.0)
    slot_s = jnp.where(fits, count + tok, -1.0)

    def spread(a):
        a = jnp.broadcast_to(a[:, None, :], (experts, SUB, tokens))
        return a.reshape(experts * SUB, tokens)

    place = (iota((experts * SUB, tokens), 0) & (SUB - 1)).astype(F32)
    put_r = spread(slot_r) == place
    put_s = jnp.where(spread(slot_s) == place, 1.0, 0.0)
    mix[...] = jnp.where(put_r, spread(gains), put_s)
    wide_r[...] = jnp.zeros_like(wide_r)
    wide_s[...] = jnp.ones_like(wide_s)
    wide_r[:, :width] = routed_in[...]
    wide_s[:, :width] = shared_in[...]
    sent = dot(jnp.where(put_r, 1.0, 0.0).astype(BF16), wide_r[...])
    sent = sent + dot(put_s.astype(BF16), wide_s[...])
    out[...] = sent.astype(BF16)


def up_body(cap, chunks, arrived, gate_w, up_w, shared_gate, shared_up, out, flags, left, right):
    padded, wide = arrived.shape
    width, units = gate_w.shape
    rows = padded // SUB * cap
    half = rows // 2
    compact = dot(pick_rows(rows, padded, cap), arrived[...])
    shared = compact[:, width : width + 1] > 0.5
    flags[...] = jnp.broadcast_to(jnp.where(shared, 1.0, 0.0), flags.shape)
    left[...] = jnp.where(shared, 0.0, compact).astype(BF16)[:, :width]
    right[...] = jnp.where(shared, compact, 0.0).astype(BF16)[:, :width]
    odd = lax.axis_index("expert") % 2 == 1
    step = 2 * LANES
    for c in range(units // step):
        cols = slice(c * step, (c + 1) * step)
        for which, (w, s) in enumerate(((gate_w, shared_gate), (up_w, shared_up))):
            value = dot(left[...], w[:, cols]) + dot(right[...], s[:, cols])
            value = value.astype(BF16)
            for b in range(2):
                for j in range(2):
                    owner = 2 * (2 * c + b) + j
                    out[jnp.where(odd, chunks[1][owner], chunks[0][owner]), which * half : (which + 1) * half, :] = value[
                        j * half : (j + 1) * half, b * LANES : (b + 1) * LANES
                    ]


def add_body(parts, out):
    for q in range(out.shape[0]):
        total = parts[0, q].astype(F32)
        for s in range(1, parts.shape[0]):
            total = total + parts[s, q].astype(F32)
        out[q] = total.astype(BF16)


def act_body(parts, out):
    sources, both, _ = parts.shape
    half = both // 2
    gate = jnp.zeros((half, LANES), F32)
    upper = jnp.zeros((half, LANES), F32)
    for s in range(sources):
        gate = gate + parts[s, :half, :].astype(F32)
        upper = upper + parts[s, half:, :].astype(F32)
    hidden = (jax.nn.silu(gate) * upper).astype(BF16)
    for s in range(out.shape[0]):
        out[s] = hidden


def down_body(cap, hidden, flags, down_t, shared_down_t, out, joined):
    owners, half, _ = hidden.shape
    padded = out.shape[0]
    rows = 2 * half
    for owner in range(owners):
        i, j = owner // 2, owner % 2
        joined[j * half : (j + 1) * half, i * LANES : (i + 1) * LANES] = hidden[owner]
    last = ((1,), (1,))
    own = dot(joined[...], down_t[...], last)
    common = dot(joined[...], shared_down_t[...], last)
    value = jnp.where(flags[:, :1] > 0.5, common, own).astype(BF16)
    out[...] = dot(pick_rows(rows, padded, cap), value, ((0,), (0,))).astype(BF16)


def mix_body(returned, mix, out):
    value = dot(mix[...], returned[...].astype(F32), ((0,), (0,)), lax.Precision.HIGHEST)
    out[...] = value.astype(BF16)


def call(body, shape, dtype, *args, scratch=(), in_hbm=0, flops=0):
    several = isinstance(dtype, tuple)
    outs = [jax.ShapeDtypeStruct(a, d) for a, d in zip(shape, dtype)] if several else jax.ShapeDtypeStruct(shape, dtype)
    hbm, vmem = pl.BlockSpec(memory_space=pltpu.HBM), pl.BlockSpec(memory_space=pltpu.VMEM)
    return pl.pallas_call(
        body,
        out_shape=outs,
        in_specs=[hbm if n < in_hbm else vmem for n in range(len(args))],
        scratch_shapes=list(scratch),
        compiler_params=pltpu.CompilerParams(vmem_limit_bytes=GRANT),
        cost_estimate=pl.CostEstimate(flops=flops, bytes_accessed=0, transcendentals=0) if flops else None,
    )(*[pltpu.with_memory_space_constraint(a, pltpu.HBM) if n < in_hbm else a for n, a in enumerate(args)])


def stage_groups(owners, experts):
    down, across = owners // NEAR, NEAR
    assert down == 2 * NEAR and across == NEAR
    stages = ([], [])
    chunks = [[0] * owners, [0] * owners]
    for e in range(experts):
        if e % 2 == 0:
            one = [[(y, x) for x in range(across)] for y in range(down)]
            two = [[(y, x) for y in range(down)] for x in range(across)]
        else:
            one = [[(y, x) for y in line] for line in RING for x in range(across)]
            two = [[(y, x) for y in pair for x in range(across)] for pair in zip(*RING)]
        place = [{d: group.index(d) for group in stage for d in group} for stage in (one, two)]
        for y in range(down):
            for x in range(across):
                a, b = (p[y, x] for p in place)
                chunks[e % 2][y * across + x] = a * down + b
        for groups, stage in zip(stages, (one, two)):
            groups += [[(y * across + x) * experts + e for y, x in group] for group in stage]
    return stages, chunks


def exchange(array, groups):
    return lax.all_to_all(array, ("dp", "expert"), 0, 0, tiled=True, axis_index_groups=groups)


def local(
    shortcut_in,
    current_in,
    expert_ids,
    route_weight,
    gate_weight,
    up_weight,
    down_weight,
    shared_gate,
    shared_up,
    shared_down,
):
    sources = lax.axis_size("expert")
    owners = lax.axis_size("dp")
    tokens, top = expert_ids.shape
    cap = 3 * tokens * top // (2 * sources)
    width = shortcut_in.shape[1]
    units = gate_weight.shape[2]
    padded = sources * SUB
    rows = sources * cap
    sent, mix = call(
        lambda *r: pack_body(cap, *r),
        ((padded, WIDE), (padded, tokens)),
        (BF16, F32),
        expert_ids.T,
        route_weight.T,
        shortcut_in,
        current_in,
        in_hbm=4,
        flops=EARLY,
        scratch=(
            pltpu.VMEM((top, tokens), jnp.int32),
            pltpu.VMEM((top, tokens), F32),
            pltpu.VMEM((tokens, width), BF16),
            pltpu.VMEM((tokens, width), BF16),
            pltpu.VMEM((tokens, WIDE), BF16),
            pltpu.VMEM((tokens, WIDE), BF16),
            pltpu.SemaphoreType.DMA((4,)),
        ),
    )
    arrived = lax.all_to_all(sent.reshape(sources, SUB, WIDE), "expert", 0, 0, tiled=True)
    arrived = arrived.reshape(padded, WIDE)
    (one, two), chunks = stage_groups(owners, sources)
    parts, flags = call(
        lambda *r: up_body(cap, chunks, *r),
        ((owners, rows, LANES), (rows, LANES)),
        (BF16, F32),
        arrived,
        gate_weight[0],
        up_weight[0],
        shared_gate,
        shared_up,
        scratch=(pltpu.VMEM((rows, width), BF16), pltpu.VMEM((rows, width), BF16)),
    )
    left = owners // NEAR
    parts = exchange(parts.reshape(NEAR, left * rows, LANES), one)
    parts = call(add_body, (left, rows, LANES), BF16, parts.reshape(NEAR, left, rows, LANES))
    parts = exchange(parts, two)
    copies = call(act_body, (owners, rows // 2, LANES), BF16, parts)
    hidden = lax.all_to_all(copies, "dp", 0, 0, tiled=True)
    results = call(
        lambda *r: down_body(cap, *r),
        (padded, width),
        BF16,
        hidden,
        flags,
        down_weight[0].T,
        shared_down.T,
        scratch=(pltpu.VMEM((rows, units), BF16),),
    )
    returned = lax.all_to_all(results.reshape(sources, SUB, width), "expert", 0, 0, tiled=True)
    return call(mix_body, (tokens, width), BF16, returned.reshape(padded, width), mix)


def solution(mesh):
    placed = (
        P("expert", "dp"),
        P("expert", "dp"),
        P("expert", None),
        P("expert", None),
        P("expert", "dp", None),
        P("expert", "dp", None),
        P("expert", None, "dp"),
        P("dp", None),
        P("dp", None),
        P(None, "dp"),
    )
    return jax.shard_map(
        local, mesh=mesh, in_specs=placed, out_specs=P("expert", "dp"), check_vma=False
    )
```
